32 devices in a mesh: seq: 8 (over y, x, core), tp: 4 (over z).
Axes of the slice: x: 2, y: 2, z: 4, core: 2. Of those that a mesh axis runs over, the one named last changes fastest.
Arguments:
- hidden: bfloat16 [4096, 4096], P('seq', 'tp'), may hold values from -6 to 6
- norm_gain: float32 [4096], P('tp'), may hold values from 0.5 to 1.5
- rank_down: bfloat16 [4096, 1024], P('tp'), may hold values from -0.09375 to 0.09375
- gate_up: bfloat16 [1024, 4096], P(None, 'tp'), may hold values from -0.1875 to 0.1875
- value_up: bfloat16 [1024, 4096], P(None, 'tp'), may hold values from -0.1875 to 0.1875
- state_up: bfloat16 [1024, 1024], P(None, 'tp'), may hold values from -0.1875 to 0.1875
- step_up: bfloat16 [1024, 64], P(None, 'tp'), may hold values from -0.1875 to 0.1875
- conv_value: float32 [4, 4096], P(None, 'tp'), may hold values from -3 to 3
- conv_state: float32 [4, 1024], P(None, 'tp'), may hold values from -3 to 3
- step_bias: float32 [64], P('tp'), may hold values from -6.9 to -2.3
- decay_log: float32 [64], P('tp'), may hold values from -11 to 2.77
- skip_gain: float32 [64], P('tp'), may hold values from 0.5 to 1.5
- gate_gain: float32 [4096], P('tp'), may hold values from 0.5 to 1.5
- out_down: bfloat16 [4096, 1024], P('tp'), may hold values from -0.09375 to 0.09375
- out_up: bfloat16 [1024, 4096], P(None, 'tp'), may hold values from -0.1875 to 0.1875
Outputs:
- block_out: bfloat16 [4096, 4096], P('seq', 'tp')
The draws below stay inside these ranges and needn't reach their ends.
All inputs are finite; a program needn't handle non-finite values.
Results may differ from the reference program's by a relative error of at most 0.012.
Values may be sent and summed in bfloat16 or wider, within the bound.
A program may use at most 64 MiB of HBM per device.

```python
import jax
import jax.numpy as jnp
from jax import lax

D = 4096
HEAD_DIM = 64
NSTATE = 128
CONV = 4
RANK = 1024
HEADS = 64
GROUPS = 4
TOK_DEV = 512
INNER = 4096
SEQ_LEN = 4096


def levels(rng, extent, cuts, low, largest):
    level = 1.0
    for position, blocks in cuts:
        steps = jax.random.uniform(jax.random.fold_in(jax.random.fold_in(rng, 6), position), (blocks,), jnp.float32, low / len(cuts), largest / len(cuts))
        level = level * jnp.repeat(jnp.exp(steps), extent[position] // blocks).reshape((-1,) + (1,) * (len(extent) - 1 - position))
    return level


def noise(own_key, extent, deviation, reach, split=(), kind=jnp.bfloat16):
    values = deviation * jax.random.normal(own_key, extent, jnp.float32)
    if split:
        values = values * levels(own_key, extent, split, -0.22, 0.18)
    return jnp.clip(values, -reach, reach).astype(kind)


def setup_inputs(seed: int = 0) -> dict:
    key_list = jax.random.split(jax.random.key(seed), 16)
    hidden = noise(key_list[0], (SEQ_LEN, D), 1.0, 6.0, ((0, 8), (1, 4)))
    norm_gain = jnp.clip(1.0 + 0.1 * jax.random.normal(key_list[1], (D,), jnp.float32), 0.5, 1.5)
    rank_down = noise(key_list[2], (D, RANK), D ** -0.5, 0.09375, ((0, 4),))
    gate_up = noise(key_list[3], (RANK, INNER), RANK ** -0.5, 0.1875, ((1, 4),))
    value_up = noise(key_list[4], (RANK, INNER), RANK ** -0.5, 0.1875, ((1, 4),))
    state_up = noise(key_list[5], (RANK, 2 * GROUPS * NSTATE), RANK ** -0.5, 0.1875, ((1, 4),))
    step_up = noise(key_list[6], (RANK, HEADS), RANK ** -0.5, 0.1875, ((1, 4),))
    conv_value = noise(key_list[7], (CONV, INNER), CONV ** -0.5, 3.0, ((1, 4),), jnp.float32)
    conv_state = noise(key_list[8], (CONV, 2 * GROUPS * NSTATE), CONV ** -0.5, 3.0, ((1, 4),), jnp.float32)
    step_bias = jnp.clip(-6.9 + 4.6000001430511475 * jax.random.uniform(key_list[9], (HEADS,), jnp.float32) ** levels(key_list[9], (HEADS,), ((0, 4),), -0.2, 0.2), -6.9, -2.3)
    decay_log = jnp.clip(-11.0 + 13.77 * jax.random.uniform(key_list[10], (HEADS,), jnp.float32) ** levels(key_list[10], (HEADS,), ((0, 4),), -0.2, 0.2), -11.0, 2.77)
    skip_gain = jnp.clip(0.5 + 1.0 * jax.random.uniform(key_list[11], (HEADS,), jnp.float32) ** levels(key_list[11], (HEADS,), ((0, 4),), -0.2, 0.2), 0.5, 1.5)
    gate_gain = jnp.clip(1.0 + 0.1 * jax.random.normal(key_list[12], (INNER,), jnp.float32), 0.5, 1.5)
    out_down = noise(key_list[13], (INNER, RANK), INNER ** -0.5, 0.09375, ((0, 4),))
    out_up = noise(key_list[14], (RANK, D), RANK ** -0.5, 0.1875, ((1, 4),))
    return {"hidden": hidden, "norm_gain": norm_gain, "rank_down": rank_down, "gate_up": gate_up, "value_up": value_up, "state_up": state_up, "step_up": step_up, "conv_value": conv_value, "conv_state": conv_state, "step_bias": step_bias, "decay_log": decay_log, "skip_gain": skip_gain, "gate_gain": gate_gain, "out_down": out_down, "out_up": out_up}


epsilon = 1e-05
highest = lax.Precision.HIGHEST

def depthwise(pre_rows, weights):
    padded = jnp.pad(pre_rows.astype(jnp.float32), ((CONV - 1, 0), (0, 0)))
    length = pre_rows.shape[0]
    result = jnp.zeros(pre_rows.shape, jnp.float32)
    for offset in range(CONV):
        result = result + weights[offset] * padded[offset:offset + length]
    return jax.nn.silu(result).astype(jnp.bfloat16)

def reference(hidden, norm_gain, rank_down, gate_up, value_up, state_up, step_up, conv_value, conv_state, step_bias, decay_log, skip_gain, gate_gain, out_down, out_up):
    blocks = SEQ_LEN // TOK_DEV
    hidden_blocks = hidden.reshape(blocks, TOK_DEV, D)

    def in_block(rows):
        wide_rows = rows.astype(jnp.float32)
        factor = lax.rsqrt(lax.optimization_barrier(jnp.mean(wide_rows * wide_rows, axis=1)) + epsilon)
        scaled = (wide_rows * norm_gain).astype(jnp.bfloat16)
        reduced = (jnp.dot(scaled, rank_down, preferred_element_type=jnp.float32) * factor[:, None]).astype(jnp.bfloat16)
        return tuple((jnp.dot(reduced, weight, preferred_element_type=jnp.float32).astype(jnp.bfloat16) for weight in (gate_up, value_up, state_up, step_up)))
    gate_pre, value_pre, state_pre, step_pre = lax.map(in_block, hidden_blocks)
    value_act = depthwise(value_pre.reshape(SEQ_LEN, INNER), conv_value)
    state_act = depthwise(state_pre.reshape(SEQ_LEN, 2 * GROUPS * NSTATE), conv_state)
    repeat_count = HEADS // GROUPS
    causal = jnp.arange(TOK_DEV)[:, None] >= jnp.arange(TOK_DEV)[None, :]

    def ssd_block(state, inputs):
        value_rows, state_rows, step_rows = inputs
        step_size = jax.nn.softplus(step_rows.astype(jnp.float32) + step_bias)
        log_decay = jnp.cumsum(-jnp.exp(decay_log) * step_size, axis=0)
        values = value_rows.astype(jnp.float32).reshape(TOK_DEV, HEADS, HEAD_DIM)
        projections = state_rows.astype(jnp.float32)
        inward = projections[:, :GROUPS * NSTATE].reshape(TOK_DEV, GROUPS, NSTATE)
        outward = projections[:, GROUPS * NSTATE:].reshape(TOK_DEV, GROUPS, NSTATE)
        inward_heads = jnp.repeat(inward, repeat_count, axis=1)
        outward_heads = jnp.repeat(outward, repeat_count, axis=1)
        coupling = jnp.einsum('tgn,sgn->gts', outward, inward, precision=highest)
        coupling = jnp.repeat(coupling, repeat_count, axis=0)
        spread = log_decay.T[:, :, None] - log_decay.T[:, None, :]
        attenuation = jnp.where(causal[None], jnp.exp(jnp.where(causal[None], spread, 0.0)), 0.0)
        mixing = coupling * attenuation * step_size.T[:, None, :]
        within = jnp.einsum('hts,shp->thp', mixing, values, precision=highest)
        carried_in = jnp.exp(log_decay)[:, :, None] * jnp.einsum('thn,hpn->thp', outward_heads, state, precision=highest)
        mixed = within + carried_in + skip_gain[None, :, None] * values
        ending = jnp.exp(log_decay[-1][None, :] - log_decay) * step_size
        new_state = jnp.exp(log_decay[-1])[:, None, None] * state + jnp.einsum('sh,shp,shn->hpn', ending, values, inward_heads, precision=highest)
        return (new_state, mixed.reshape(TOK_DEV, INNER))
    start_state = jnp.zeros((HEADS, HEAD_DIM, NSTATE), jnp.float32)
    scan_inputs = (value_act.reshape(blocks, TOK_DEV, INNER), state_act.reshape(blocks, TOK_DEV, 2 * GROUPS * NSTATE), step_pre)
    final_state, mixed_blocks = lax.scan(ssd_block, start_state, scan_inputs)

    def out_block(inputs):
        mixed, gate_rows, rows = inputs
        gated = mixed * jax.nn.silu(gate_rows.astype(jnp.float32))
        grouped = gated.reshape(TOK_DEV, GROUPS, INNER // GROUPS)
        factor = lax.rsqrt(lax.optimization_barrier(jnp.mean(grouped * grouped, axis=2)) + epsilon)
        normed = ((grouped * factor[:, :, None]).reshape(TOK_DEV, INNER) * gate_gain).astype(jnp.bfloat16)
        projected = jnp.dot(normed, out_down, preferred_element_type=jnp.float32).astype(jnp.bfloat16)
        update = jnp.dot(projected, out_up, preferred_element_type=jnp.float32)
        return (rows.astype(jnp.float32) + update).astype(jnp.bfloat16)
    outputs = lax.map(out_block, (mixed_blocks, gate_pre, hidden_blocks))
    return outputs.reshape(SEQ_LEN, D)
```

```python
import functools

import jax
import jax.numpy as jnp
from jax import lax
from jax.experimental import pallas as pl
from jax.experimental.pallas import tpu as pltpu
from jax.sharding import PartitionSpec as P

HEAD_DIM = 64
NSTATE = 128
GROUPS = 4

epsilon = 1e-05
MESH = pl.DeviceIdType.MESH
VMEM_LIMIT = 56 * 1024 * 1024


def greet(axis, offsets):
    count = lax.axis_size(axis)
    me = lax.axis_index(axis)
    barrier = pltpu.get_barrier_semaphore()
    for offset in offsets:
        pl.semaphore_signal(
            barrier, inc=1, device_id={axis: lax.rem(me + offset, count)}, device_id_type=MESH
        )
    pl.semaphore_wait(barrier, len(offsets))


def send(source, target, send_sem, recv_sem, axis, peer):
    copy = pltpu.make_async_remote_copy(
        src_ref=source,
        dst_ref=target,
        send_sem=send_sem,
        recv_sem=recv_sem,
        device_id={axis: peer},
        device_id_type=MESH,
    )
    copy.start()
    return copy


def project_kernel(
    n, with_norm, width, *refs
):
    if with_norm:
        (rows_ref, gain_ref, weight_ref, out_ref, parts, arrived, own, sq_parts, sq_arrived,
         part_send, part_recv, sq_send, sq_recv, full_send, full_recv) = refs
    else:
        (rows_ref, weight_ref, out_ref, parts, arrived, own,
         part_send, part_recv, full_send, full_recv) = refs
    me = lax.axis_index("tp")
    length = rows_ref.shape[0] // n
    greet("tp", range(1, n))
    copies = []
    own_squares = None
    order = [o for o in sorted(range(1, n), key=lambda o: -min(o, n - o))] + [0]
    for offset in order:
        peer = lax.rem(me + offset, n)
        start = pl.multiple_of(peer * length, length)
        rows = rows_ref[pl.ds(start, length), :]
        if with_norm:
            wide = rows.astype(jnp.float32)
            squares = jnp.sum(wide * wide, axis=1, keepdims=True)
            rows = (wide * gain_ref[...]).astype(jnp.bfloat16)
            if offset:
                spread = jnp.broadcast_to(squares, (length, 128))
                sq_parts[offset - 1] = spread.T[:8]
                copies.append(
                    send(sq_parts.at[offset - 1], sq_arrived.at[offset - 1],
                         sq_send.at[offset - 1], sq_recv.at[offset - 1], "tp", peer)
                )
            else:
                own_squares = squares
        part = jnp.dot(rows, weight_ref[...], preferred_element_type=jnp.float32)
        if offset:
            parts[offset - 1] = part.astype(jnp.bfloat16)
            copies.append(
                send(parts.at[offset - 1], arrived.at[offset - 1],
                     part_send.at[offset - 1], part_recv.at[offset - 1], "tp", peer)
            )
        else:
            own[...] = part
    for copy in copies:
        copy.wait_recv()
    total = own[...]
    for offset in range(1, n):
        total = total + arrived[offset - 1].astype(jnp.float32)
    if with_norm:
        others = sq_arrived[0]
        for offset in range(2, n):
            others = others + sq_arrived[offset - 1]
        column = jnp.broadcast_to(others[:1], (128, length)).T[:, :1]
        factor = lax.rsqrt((own_squares + column) / width + epsilon)
        total = total * factor
    mine = pl.multiple_of(me * length, length)
    out_ref[pl.ds(mine, length), :] = total.astype(jnp.bfloat16)
    full = [
        send(out_ref.at[pl.ds(mine, length), :], out_ref.at[pl.ds(mine, length), :],
             full_send.at[offset - 1], full_recv.at[offset - 1], "tp", lax.rem(me + offset, n))
        for offset in order[:-1]
    ]
    for copy in full:
        copy.wait_recv()
    for copy in copies + full:
        copy.wait_send()


def project(rows, weight, gain, width, collective_id):
    n = lax.axis_size("tp")
    tokens = rows.shape[0]
    length, rank = tokens // n, weight.shape[1]
    vmem = pl.BlockSpec(memory_space=pltpu.VMEM)
    sems = pltpu.SemaphoreType.DMA((n - 1,))
    with_norm = gain is not None
    scratch = [
        pltpu.VMEM((n - 1, length, rank), jnp.bfloat16),
        pltpu.VMEM((n - 1, length, rank), jnp.bfloat16),
        pltpu.VMEM((length, rank), jnp.float32),
    ]
    if with_norm:
        scratch += [pltpu.VMEM((n - 1, 8, length), jnp.float32)] * 2
    scratch += [sems] * (6 if with_norm else 4)
    operands = (rows, gain[None], weight) if with_norm else (rows, weight)
    return pl.pallas_call(
        functools.partial(project_kernel, n, with_norm, width),
        out_shape=jax.ShapeDtypeStruct((tokens, rank), jnp.bfloat16),
        in_specs=[vmem] * len(operands),
        out_specs=vmem,
        scratch_shapes=scratch,
        compiler_params=pltpu.CompilerParams(
            collective_id=collective_id, has_side_effects=True, vmem_limit_bytes=VMEM_LIMIT
        ),
    )(*operands)


def exchange_kernel(n, share, act_ref, out_ref, sends, recvs, local_sem):
    me = lax.axis_index("tp")
    columns = act_ref.shape[1]
    piece = out_ref.shape[2]
    pieces, slots = columns // piece, out_ref.shape[0]
    greet("tp", range(1, n))

    def place(index):
        column = index * piece
        side = column // (GROUPS * NSTATE)
        within = column - side * (GROUPS * NSTATE)
        group = within // NSTATE
        slot = side * (NSTATE // piece) + (within - group * NSTATE) // piece
        return group, slot

    def remote(k, r, target, slot):
        return pltpu.make_async_remote_copy(
            src_ref=act_ref.at[:, pl.ds(k * piece, piece)],
            dst_ref=out_ref.at[slot],
            send_sem=sends.at[k * share + r],
            recv_sem=recvs.at[slot],
            device_id={"tp": target},
            device_id_type=MESH,
        )

    for k in range(pieces):
        group, slot = place(me * pieces + k)
        for r in range(share):
            target = group * share + r

            @pl.when(target != me)
            def _():
                remote(k, r, target, slot).start()

            @pl.when(target == me)
            def _():
                local = pltpu.make_async_copy(
                    act_ref.at[:, pl.ds(k * piece, piece)], out_ref.at[slot], local_sem
                )
                local.start()
                local.wait()

    mine = me // share
    per_side = NSTATE // piece
    for slot in range(slots):
        side = slot // per_side
        source = (side * GROUPS * per_side + mine * per_side + slot % per_side) // pieces

        @pl.when(source != me)
        def _():
            remote(0, 0, me, slot).wait_recv()

    for k in range(pieces):
        group, slot = place(me * pieces + k)
        for r in range(share):

            @pl.when(group * share + r != me)
            def _():
                remote(k, r, group * share + r, slot).wait_send()


def exchange(act, collective_id):
    n = lax.axis_size("tp")
    tokens, columns = act.shape
    piece = min(columns, NSTATE)
    share = n // GROUPS
    slots = 2 * NSTATE // piece
    vmem = pl.BlockSpec(memory_space=pltpu.VMEM)
    return pl.pallas_call(
        functools.partial(exchange_kernel, n, share),
        out_shape=jax.ShapeDtypeStruct((slots, tokens, piece), act.dtype),
        in_specs=[vmem],
        out_specs=vmem,
        scratch_shapes=[
            pltpu.SemaphoreType.DMA((columns // piece * share,)),
            pltpu.SemaphoreType.DMA((slots,)),
            pltpu.SemaphoreType.DMA,
        ],
        compiler_params=pltpu.CompilerParams(
            collective_id=collective_id, has_side_effects=True, vmem_limit_bytes=VMEM_LIMIT
        ),
    )(act)


def shifted(shard, axis, by):
    peers = lax.axis_size(axis)
    pairs = [(i, i + by) for i in range(peers) if 0 <= i + by < peers]
    return lax.ppermute(shard, axis, pairs)


def entering(part, axis, combine, identity):
    place = lax.axis_index(axis)
    gathered = jax.tree.map(lambda a: lax.all_gather(a, axis), part)
    state = jax.tree.map(lambda a, e: jnp.zeros_like(a) + jnp.asarray(e, a.dtype), part, identity)

    def one(lap, state):
        return combine(
            state, jax.tree.map(lambda a: lax.dynamic_index_in_dim(a, lap, 0, False), gathered)
        )

    return lax.fori_loop(0, place, one, state)


def depthwise(rim_rows, current, weights):
    joined = jnp.concatenate([rim_rows, current], axis=0).astype(jnp.float32)
    length = current.shape[0]
    result = jnp.zeros(current.shape, jnp.float32)
    for offset in range(weights.shape[0]):
        result = result + weights[offset] * joined[offset : offset + length]
    return jax.nn.silu(result).astype(jnp.bfloat16)


def on_device(
    hidden,
    norm_gain,
    rank_down,
    gate_up,
    value_up,
    state_up,
    step_up,
    conv_value,
    conv_state,
    step_bias,
    decay_log,
    skip_gain,
    gate_gain,
    out_down,
    out_up,
):
    tokens = hidden.shape[0]
    tp_count = lax.axis_size("tp")
    tp_index = lax.axis_index("tp")
    model_width = hidden.shape[1] * tp_count
    up_weights = (gate_up, value_up, state_up, step_up)
    reduced = project(hidden, rank_down, norm_gain, model_width, 0)
    projected = tuple(
        (jnp.dot(reduced, weight, preferred_element_type=jnp.float32) for weight in up_weights)
    )
    gate_pre = projected[0].astype(jnp.bfloat16)
    value_pre = projected[1].astype(jnp.bfloat16)
    state_pre = projected[2].astype(jnp.bfloat16)
    step_pre = projected[3].astype(jnp.bfloat16)
    rim_start = tokens - conv_value.shape[0] + 1
    rim_value, rim_state = shifted((value_pre[rim_start:], state_pre[rim_start:]), "seq", 1)
    value_act = depthwise(rim_value, value_pre, conv_value)
    state_act = depthwise(rim_state, state_pre, conv_state)
    heads_local = decay_log.shape[0]
    heads_total = heads_local * tp_count
    group_index = tp_index * heads_local // (heads_total // GROUPS)
    sides = exchange(state_act, 1)
    half = sides.shape[0] // 2
    inward = jnp.concatenate([sides[i] for i in range(half)], axis=1)
    outward = jnp.concatenate([sides[half + i] for i in range(half)], axis=1)
    step_size = jax.nn.softplus(step_pre.astype(jnp.float32) + step_bias)
    log_decay = jnp.cumsum(-jnp.exp(decay_log) * step_size, axis=0)
    values = value_act.astype(jnp.float32).reshape(tokens, heads_local, HEAD_DIM)
    coupling = lax.dot_general(
        outward, inward, (((1,), (1,)), ((), ())), preferred_element_type=jnp.float32
    )
    positions = jnp.arange(tokens)
    causal = positions[:, None] >= positions[None, :]
    spread = log_decay.T[:, :, None] - log_decay.T[:, None, :]
    attenuation = jnp.where(causal[None], jnp.exp(jnp.where(causal[None], spread, 0.0)), 0.0)
    mixing = coupling[None] * attenuation * step_size.T[:, None, :]
    narrow_values = value_act.reshape(tokens, heads_local, HEAD_DIM)
    within = jnp.einsum(
        "hts,shp->thp",
        mixing.astype(jnp.bfloat16),
        narrow_values,
        preferred_element_type=jnp.float32,
    )
    ending = jnp.exp(log_decay[-1][None, :] - log_decay) * step_size
    weighted = (ending[:, :, None] * values).astype(jnp.bfloat16)
    local_state = jnp.einsum("shp,sn->hpn", weighted, inward, preferred_element_type=jnp.float32)
    local_decay = jnp.exp(log_decay[-1])

    def combine(earlier, later):
        return (earlier[0] * later[0], later[0][:, None, None] * earlier[1] + later[1])

    prefix = entering(
        (local_decay, local_state),
        "seq",
        combine,
        (jnp.ones_like(local_decay), jnp.zeros_like(local_state)),
    )
    incoming = prefix[1]
    carried_in = jnp.exp(log_decay)[:, :, None] * jnp.einsum(
        "tn,hpn->thp",
        outward,
        incoming.astype(jnp.bfloat16),
        preferred_element_type=jnp.float32,
    )
    mixed = (within + carried_in + skip_gain[None, :, None] * values).reshape(
        tokens, heads_local * HEAD_DIM
    )
    gated = mixed * jax.nn.silu(gate_pre.astype(jnp.float32))
    group_width = heads_total * HEAD_DIM // GROUPS
    own_sum = jnp.sum(gated * gated, axis=1)
    if heads_local * HEAD_DIM < group_width:
        selector = (jnp.arange(GROUPS) == group_index).astype(jnp.float32)
        group_sums = lax.psum(own_sum[:, None] * selector[None, :], "tp")
        own_sum = jnp.sum(group_sums * selector[None, :], axis=1)
    normed = (gated * lax.rsqrt(own_sum / group_width + epsilon)[:, None] * gate_gain).astype(
        jnp.bfloat16
    )
    shared = project(normed, out_down, None, None, 2)
    update = jnp.dot(shared, out_up, preferred_element_type=jnp.float32)
    return (hidden.astype(jnp.float32) + update).astype(jnp.bfloat16)


def solution(mesh):
    return jax.shard_map(
        on_device,
        mesh=mesh,
        in_specs=(
            P("seq", "tp"),
            P("tp"),
            P("tp", None),
            P(None, "tp"),
            P(None, "tp"),
            P(None, "tp"),
            P(None, "tp"),
            P(None, "tp"),
            P(None, "tp"),
            P("tp"),
            P("tp"),
            P("tp"),
            P("tp"),
            P("tp", None),
            P(None, "tp"),
        ),
        out_specs=P("seq", "tp"),
        check_vma=False,
    )
```

```python
import functools

import jax
import jax.numpy as jnp
from jax import lax
from jax.experimental import pallas as pl
from jax.experimental.pallas import tpu as pltpu
from jax.sharding import PartitionSpec as P

HEAD_DIM = 64
NSTATE = 128
GROUPS = 4

epsilon = 1e-05
MESH = pl.DeviceIdType.MESH
VMEM_LIMIT = 56 * 1024 * 1024


def greet(axis, offsets):
    count = lax.axis_size(axis)
    me = lax.axis_index(axis)
    barrier = pltpu.get_barrier_semaphore()
    for offset in offsets:
        pl.semaphore_signal(
            barrier, inc=1, device_id={axis: lax.rem(me + offset, count)}, device_id_type=MESH
        )
    pl.semaphore_wait(barrier, len(offsets))


def project_kernel(n, pieces, with_norm, width, *refs):
    if with_norm:
        (rows_ref, gain_ref, weight_ref, out_ref, parts, inbound, back, part_send, part_recv,
         back_recv, full_send, full_recv, squares, sq_in, sq_back, sq_send, sq_recv,
         sq_back_recv) = refs
    else:
        (rows_ref, weight_ref, out_ref, parts, inbound, back, part_send, part_recv, back_recv,
         full_send, full_recv) = refs
    me = lax.axis_index("tp")
    tokens = rows_ref.shape[0]
    length = tokens // pieces
    left = me < n // 2
    inner = jnp.where(left, me + 1, me - 1)
    outer = jnp.where(left, me - 1, me + 1)
    end = (me == 0) | (me == n - 1)
    middle = (me == n // 2 - 1) | (me == n // 2)
    outer = jnp.where(end, inner, outer)
    greet("tp", range(1, n))

    def copy(source, target, send_sem, recv_sem, peer):
        return pltpu.make_async_remote_copy(
            src_ref=source,
            dst_ref=target,
            send_sem=send_sem,
            recv_sem=recv_sem,
            device_id={"tp": peer},
            device_id_type=MESH,
        )

    def sq_into():
        return copy(squares, sq_in, sq_send, sq_recv, inner)

    def sq_across():
        return copy(squares, sq_back, sq_send, sq_back_recv, inner)

    def into(k):
        return copy(parts.at[k], inbound.at[k], part_send.at[k], part_recv.at[k], inner)

    def across(k):
        return copy(parts.at[k], back.at[k], part_send.at[k], back_recv.at[k], inner)

    def outward(k):
        rows = out_ref.at[pl.ds(k * length, length), :]
        return copy(rows, rows, full_send.at[k], full_recv.at[k], outer)

    if with_norm:
        wide = rows_ref[...].astype(jnp.float32)
        column = jnp.sum(wide * wide, axis=1, keepdims=True)
        squares[...] = jnp.broadcast_to(column, (tokens, 128)).T[:8]

        @pl.when(jnp.logical_not(end))
        def _():
            sq_into().wait_recv()
            squares[...] += sq_in[...]

        @pl.when(middle)
        def _():
            sq_across().start()

        @pl.when(jnp.logical_not(middle))
        def _():
            sq_into().start()

    def gather_part(k):
        rows = rows_ref[pl.ds(k * length, length), :]
        if with_norm:
            rows = (rows.astype(jnp.float32) * gain_ref[...]).astype(jnp.bfloat16)
        part = jnp.dot(rows, weight_ref[...], preferred_element_type=jnp.float32)

        @pl.when(end)
        def _():
            parts[k] = part.astype(jnp.bfloat16)

        @pl.when(jnp.logical_not(end))
        def _():
            into(k).wait_recv()
            parts[k] = (part + inbound[k].astype(jnp.float32)).astype(jnp.bfloat16)

        @pl.when(middle)
        def _():
            across(k).start()

        @pl.when(jnp.logical_not(middle))
        def _():
            into(k).start()

    def finish_part(k):
        @pl.when(middle)
        def _():
            across(k).wait_recv()
            total = parts[k].astype(jnp.float32) + back[k].astype(jnp.float32)
            if with_norm:
                row = squares[:1, k * length : (k + 1) * length]
                if k == 0:
                    sq_across().wait_recv()
                row = row + sq_back[:1, k * length : (k + 1) * length]
                column = jnp.broadcast_to(row, (128, length)).T[:, :1]
                total = total * lax.rsqrt(column / width + epsilon)
            out_ref[pl.ds(k * length, length), :] = total.astype(jnp.bfloat16)

        @pl.when(jnp.logical_not(middle))
        def _():
            outward(k).wait_recv()

        @pl.when(jnp.logical_not(end))
        def _():
            outward(k).start()

    lag = min(2, pieces)
    for k in range(pieces + lag):
        if k < pieces:
            gather_part(k)
        if k >= lag:
            finish_part(k - lag)
    for k in range(pieces):
        into(k).wait_send()

        @pl.when(jnp.logical_not(end))
        def _():
            outward(k).wait_send()

    if with_norm:
        sq_into().wait_send()


def project(rows, weight, gain, width, collective_id):
    n = lax.axis_size("tp")
    tokens = rows.shape[0]
    pieces = 8
    length, rank = tokens // pieces, weight.shape[1]
    vmem = pl.BlockSpec(memory_space=pltpu.VMEM)
    sems = pltpu.SemaphoreType.DMA((pieces,))
    with_norm = gain is not None
    scratch = [pltpu.VMEM((pieces, length, rank), jnp.bfloat16)] * 3 + [sems] * 5
    if with_norm:
        scratch += [pltpu.VMEM((8, tokens), jnp.float32)] * 3 + [pltpu.SemaphoreType.DMA] * 3
    operands = (rows, gain[None], weight) if with_norm else (rows, weight)
    return pl.pallas_call(
        functools.partial(project_kernel, n, pieces, with_norm, width),
        out_shape=jax.ShapeDtypeStruct((tokens, rank), jnp.bfloat16),
        in_specs=[vmem] * len(operands),
        out_specs=vmem,
        scratch_shapes=scratch,
        compiler_params=pltpu.CompilerParams(
            collective_id=collective_id, has_side_effects=True, vmem_limit_bytes=VMEM_LIMIT
        ),
    )(*operands)


def exchange_kernel(n, share, act_ref, out_ref, sends, recvs, local_sem):
    me = lax.axis_index("tp")
    columns = act_ref.shape[1]
    piece = out_ref.shape[2]
    pieces, slots = columns // piece, out_ref.shape[0]
    greet("tp", range(1, n))

    def place(index):
        column = index * piece
        side = column // (GROUPS * NSTATE)
        within = column - side * (GROUPS * NSTATE)
        group = within // NSTATE
        slot = side * (NSTATE // piece) + (within - group * NSTATE) // piece
        return group, slot

    def remote(k, r, target, slot):
        return pltpu.make_async_remote_copy(
            src_ref=act_ref.at[:, pl.ds(k * piece, piece)],
            dst_ref=out_ref.at[slot],
            send_sem=sends.at[k * share + r],
            recv_sem=recvs.at[slot],
            device_id={"tp": target},
            device_id_type=MESH,
        )

    for k in range(pieces):
        group, slot = place(me * pieces + k)
        for r in range(share):
            target = group * share + r

            @pl.when(target != me)
            def _():
                remote(k, r, target, slot).start()

            @pl.when(target == me)
            def _():
                local = pltpu.make_async_copy(
                    act_ref.at[:, pl.ds(k * piece, piece)], out_ref.at[slot], local_sem
                )
                local.start()
                local.wait()

    mine = me // share
    per_side = NSTATE // piece
    for slot in range(slots):
        side = slot // per_side
        source = (side * GROUPS * per_side + mine * per_side + slot % per_side) // pieces

        @pl.when(source != me)
        def _():
            remote(0, 0, me, slot).wait_recv()

    for k in range(pieces):
        group, slot = place(me * pieces + k)
        for r in range(share):

            @pl.when(group * share + r != me)
            def _():
                remote(k, r, group * share + r, slot).wait_send()


def exchange(act, collective_id):
    n = lax.axis_size("tp")
    tokens, columns = act.shape
    piece = min(columns, NSTATE)
    share = n // GROUPS
    slots = 2 * NSTATE // piece
    vmem = pl.BlockSpec(memory_space=pltpu.VMEM)
    return pl.pallas_call(
        functools.partial(exchange_kernel, n, share),
        out_shape=jax.ShapeDtypeStruct((slots, tokens, piece), act.dtype),
        in_specs=[vmem],
        out_specs=vmem,
        scratch_shapes=[
            pltpu.SemaphoreType.DMA((columns // piece * share,)),
            pltpu.SemaphoreType.DMA((slots,)),
            pltpu.SemaphoreType.DMA,
        ],
        compiler_params=pltpu.CompilerParams(
            collective_id=collective_id, has_side_effects=True, vmem_limit_bytes=VMEM_LIMIT
        ),
    )(act)


def shifted(shard, axis, by):
    peers = lax.axis_size(axis)
    pairs = [(i, i + by) for i in range(peers) if 0 <= i + by < peers]
    return lax.ppermute(shard, axis, pairs)


def entering(part, axis, combine, identity):
    place = lax.axis_index(axis)
    gathered = jax.tree.map(lambda a: lax.all_gather(a, axis), part)
    state = jax.tree.map(lambda a, e: jnp.zeros_like(a) + jnp.asarray(e, a.dtype), part, identity)

    def one(lap, state):
        return combine(
            state, jax.tree.map(lambda a: lax.dynamic_index_in_dim(a, lap, 0, False), gathered)
        )

    return lax.fori_loop(0, place, one, state)


def depthwise(rim_rows, current, weights):
    joined = jnp.concatenate([rim_rows, current], axis=0).astype(jnp.float32)
    length = current.shape[0]
    result = jnp.zeros(current.shape, jnp.float32)
    for offset in range(weights.shape[0]):
        result = result + weights[offset] * joined[offset : offset + length]
    return jax.nn.silu(result).astype(jnp.bfloat16)


def on_device(
    hidden,
    norm_gain,
    rank_down,
    gate_up,
    value_up,
    state_up,
    step_up,
    conv_value,
    conv_state,
    step_bias,
    decay_log,
    skip_gain,
    gate_gain,
    out_down,
    out_up,
):
    tokens = hidden.shape[0]
    tp_count = lax.axis_size("tp")
    tp_index = lax.axis_index("tp")
    model_width = hidden.shape[1] * tp_count
    up_weights = (gate_up, value_up, state_up, step_up)
    reduced = project(hidden, rank_down, norm_gain, model_width, 0)
    projected = tuple(
        (jnp.dot(reduced, weight, preferred_element_type=jnp.float32) for weight in up_weights)
    )
    gate_pre = projected[0].astype(jnp.bfloat16)
    value_pre = projected[1].astype(jnp.bfloat16)
    state_pre = projected[2].astype(jnp.bfloat16)
    step_pre = projected[3].astype(jnp.bfloat16)
    rim_start = tokens - conv_value.shape[0] + 1
    rim_value, rim_state = shifted((value_pre[rim_start:], state_pre[rim_start:]), "seq", 1)
    value_act = depthwise(rim_value, value_pre, conv_value)
    state_act = depthwise(rim_state, state_pre, conv_state)
    heads_local = decay_log.shape[0]
    heads_total = heads_local * tp_count
    group_index = tp_index * heads_local // (heads_total // GROUPS)
    sides = exchange(state_act, 1)
    half = sides.shape[0] // 2
    inward = jnp.concatenate([sides[i] for i in range(half)], axis=1)
    outward = jnp.concatenate([sides[half + i] for i in range(half)], axis=1)
    step_size = jax.nn.softplus(step_pre.astype(jnp.float32) + step_bias)
    log_decay = jnp.cumsum(-jnp.exp(decay_log) * step_size, axis=0)
    values = value_act.astype(jnp.float32).reshape(tokens, heads_local, HEAD_DIM)
    coupling = lax.dot_general(
        outward, inward, (((1,), (1,)), ((), ())), preferred_element_type=jnp.float32
    )
    positions = jnp.arange(tokens)
    causal = positions[:, None] >= positions[None, :]
    spread = log_decay.T[:, :, None] - log_decay.T[:, None, :]
    attenuation = jnp.where(causal[None], jnp.exp(jnp.where(causal[None], spread, 0.0)), 0.0)
    mixing = coupling[None] * attenuation * step_size.T[:, None, :]
    narrow_values = value_act.reshape(tokens, heads_local, HEAD_DIM)
    within = jnp.einsum(
        "hts,shp->thp",
        mixing.astype(jnp.bfloat16),
        narrow_values,
        preferred_element_type=jnp.float32,
    )
    ending = jnp.exp(log_decay[-1][None, :] - log_decay) * step_size
    weighted = (ending[:, :, None] * values).astype(jnp.bfloat16)
    local_state = jnp.einsum("shp,sn->hpn", weighted, inward, preferred_element_type=jnp.float32)
    local_decay = jnp.exp(log_decay[-1])

    def combine(earlier, later):
        return (earlier[0] * later[0], later[0][:, None, None] * earlier[1] + later[1])

    prefix = entering(
        (local_decay, local_state),
        "seq",
        combine,
        (jnp.ones_like(local_decay), jnp.zeros_like(local_state)),
    )
    incoming = prefix[1]
    carried_in = jnp.exp(log_decay)[:, :, None] * jnp.einsum(
        "tn,hpn->thp",
        outward,
        incoming.astype(jnp.bfloat16),
        preferred_element_type=jnp.float32,
    )
    mixed = (within + carried_in + skip_gain[None, :, None] * values).reshape(
        tokens, heads_local * HEAD_DIM
    )
    gated = mixed * jax.nn.silu(gate_pre.astype(jnp.float32))
    group_width = heads_total * HEAD_DIM // GROUPS
    own_sum = jnp.sum(gated * gated, axis=1)
    if heads_local * HEAD_DIM < group_width:
        selector = (jnp.arange(GROUPS) == group_index).astype(jnp.float32)
        group_sums = lax.psum(own_sum[:, None] * selector[None, :], "tp")
        own_sum = jnp.sum(group_sums * selector[None, :], axis=1)
    normed = (gated * lax.rsqrt(own_sum / group_width + epsilon)[:, None] * gate_gain).astype(
        jnp.bfloat16
    )
    shared = project(normed, out_down, None, None, 2)
    update = jnp.dot(shared, out_up, preferred_element_type=jnp.float32)
    return (hidden.astype(jnp.float32) + update).astype(jnp.bfloat16)


def solution(mesh):
    return jax.shard_map(
        on_device,
        mesh=mesh,
        in_specs=(
            P("seq", "tp"),
            P("tp"),
            P("tp", None),
            P(None, "tp"),
            P(None, "tp"),
            P(None, "tp"),
            P(None, "tp"),
            P(None, "tp"),
            P(None, "tp"),
            P("tp"),
            P("tp"),
            P("tp"),
            P("tp"),
            P("tp", None),
            P(None, "tp"),
        ),
        out_specs=P("seq", "tp"),
        check_vma=False,
    )
```

```python
import functools

import jax
import jax.numpy as jnp
from jax import lax
from jax.experimental import pallas as pl
from jax.experimental.pallas import tpu as pltpu
from jax.sharding import PartitionSpec as P

HEAD_DIM = 64
NSTATE = 128
GROUPS = 4

epsilon = 1e-05
MESH = pl.DeviceIdType.MESH
VMEM_LIMIT = 56 * 1024 * 1024


def greet(axis, offsets):
    count = lax.axis_size(axis)
    me = lax.axis_index(axis)
    barrier = pltpu.get_barrier_semaphore()
    for offset in offsets:
        pl.semaphore_signal(
            barrier, inc=1, device_id={axis: lax.rem(me + offset, count)}, device_id_type=MESH
        )
    pl.semaphore_wait(barrier, len(offsets))


def send(source, target, send_sem, recv_sem, axis, peer):
    copy = pltpu.make_async_remote_copy(
        src_ref=source,
        dst_ref=target,
        send_sem=send_sem,
        recv_sem=recv_sem,
        device_id={axis: peer},
        device_id_type=MESH,
    )
    copy.start()
    return copy


def project_kernel(
    n, with_norm, width, *refs
):
    if with_norm:
        (rows_ref, gain_ref, weight_ref, out_ref, parts, arrived, own, sq_parts, sq_arrived,
         part_send, part_recv, sq_send, sq_recv, full_send, full_recv) = refs
    else:
        (rows_ref, weight_ref, out_ref, parts, arrived, own,
         part_send, part_recv, full_send, full_recv) = refs
    me = lax.axis_index("tp")
    length = rows_ref.shape[0] // n
    greet("tp", range(1, n))
    copies = []
    own_squares = None
    order = [o for o in sorted(range(1, n), key=lambda o: -min(o, n - o))] + [0]
    for offset in order:
        peer = lax.rem(me + offset, n)
        start = pl.multiple_of(peer * length, length)
        rows = rows_ref[pl.ds(start, length), :]
        if with_norm:
            wide = rows.astype(jnp.float32)
            squares = jnp.sum(wide * wide, axis=1, keepdims=True)
            rows = (wide * gain_ref[...]).astype(jnp.bfloat16)
            if offset:
                spread = jnp.broadcast_to(squares, (length, 128))
                sq_parts[offset - 1] = spread.T[:8]
                copies.append(
                    send(sq_parts.at[offset - 1], sq_arrived.at[offset - 1],
                         sq_send.at[offset - 1], sq_recv.at[offset - 1], "tp", peer)
                )
            else:
                own_squares = squares
        part = jnp.dot(rows, weight_ref[...], preferred_element_type=jnp.float32)
        if offset:
            parts[offset - 1] = part.astype(jnp.bfloat16)
            copies.append(
                send(parts.at[offset - 1], arrived.at[offset - 1],
                     part_send.at[offset - 1], part_recv.at[offset - 1], "tp", peer)
            )
        else:
            own[...] = part
    for copy in copies:
        copy.wait_recv()
    total = own[...]
    for offset in range(1, n):
        total = total + arrived[offset - 1].astype(jnp.float32)
    if with_norm:
        others = sq_arrived[0]
        for offset in range(2, n):
            others = others + sq_arrived[offset - 1]
        column = jnp.broadcast_to(others[:1], (128, length)).T[:, :1]
        factor = lax.rsqrt((own_squares + column) / width + epsilon)
        total = total * factor
    mine = pl.multiple_of(me * length, length)
    out_ref[pl.ds(mine, length), :] = total.astype(jnp.bfloat16)
    full = [
        send(out_ref.at[pl.ds(mine, length), :], out_ref.at[pl.ds(mine, length), :],
             full_send.at[offset - 1], full_recv.at[offset - 1], "tp", lax.rem(me + offset, n))
        for offset in order[:-1]
    ]
    for copy in full:
        copy.wait_recv()
    for copy in copies + full:
        copy.wait_send()


def project(rows, weight, gain, width, collective_id):
    n = lax.axis_size("tp")
    tokens = rows.shape[0]
    length, rank = tokens // n, weight.shape[1]
    vmem = pl.BlockSpec(memory_space=pltpu.VMEM)
    sems = pltpu.SemaphoreType.DMA((n - 1,))
    with_norm = gain is not None
    scratch = [
        pltpu.VMEM((n - 1, length, rank), jnp.bfloat16),
        pltpu.VMEM((n - 1, length, rank), jnp.bfloat16),
        pltpu.VMEM((length, rank), jnp.float32),
    ]
    if with_norm:
        scratch += [pltpu.VMEM((n - 1, 8, length), jnp.float32)] * 2
    scratch += [sems] * (6 if with_norm else 4)
    operands = (rows, gain[None], weight) if with_norm else (rows, weight)
    return pl.pallas_call(
        functools.partial(project_kernel, n, with_norm, width),
        out_shape=jax.ShapeDtypeStruct((tokens, rank), jnp.bfloat16),
        in_specs=[vmem] * len(operands),
        out_specs=vmem,
        scratch_shapes=scratch,
        compiler_params=pltpu.CompilerParams(
            collective_id=collective_id, has_side_effects=True, vmem_limit_bytes=VMEM_LIMIT
        ),
    )(*operands)


def exchange_kernel(n, share, act_ref, out_ref, sends, recvs, local_sem):
    me = lax.axis_index("tp")
    columns = act_ref.shape[1]
    piece = out_ref.shape[2]
    pieces, slots = columns // piece, out_ref.shape[0]
    greet("tp", range(1, n))

    def place(index):
        column = index * piece
        side = column // (GROUPS * NSTATE)
        within = column - side * (GROUPS * NSTATE)
        group = within // NSTATE
        slot = side * (NSTATE // piece) + (within - group * NSTATE) // piece
        return group, slot

    def remote(k, r, target, slot):
        return pltpu.make_async_remote_copy(
            src_ref=act_ref.at[:, pl.ds(k * piece, piece)],
            dst_ref=out_ref.at[slot],
            send_sem=sends.at[k * share + r],
            recv_sem=recvs.at[slot],
            device_id={"tp": target},
            device_id_type=MESH,
        )

    for k in range(pieces):
        group, slot = place(me * pieces + k)
        for r in range(share):
            target = group * share + r

            @pl.when(target != me)
            def _():
                remote(k, r, target, slot).start()

            @pl.when(target == me)
            def _():
                local = pltpu.make_async_copy(
                    act_ref.at[:, pl.ds(k * piece, piece)], out_ref.at[slot], local_sem
                )
                local.start()
                local.wait()

    mine = me // share
    per_side = NSTATE // piece
    for slot in range(slots):
        side = slot // per_side
        source = (side * GROUPS * per_side + mine * per_side + slot % per_side) // pieces

        @pl.when(source != me)
        def _():
            remote(0, 0, me, slot).wait_recv()

    for k in range(pieces):
        group, slot = place(me * pieces + k)
        for r in range(share):

            @pl.when(group * share + r != me)
            def _():
                remote(k, r, group * share + r, slot).wait_send()


def exchange(act, collective_id):
    n = lax.axis_size("tp")
    tokens, columns = act.shape
    piece = min(columns, NSTATE)
    share = n // GROUPS
    slots = 2 * NSTATE // piece
    vmem = pl.BlockSpec(memory_space=pltpu.VMEM)
    return pl.pallas_call(
        functools.partial(exchange_kernel, n, share),
        out_shape=jax.ShapeDtypeStruct((slots, tokens, piece), act.dtype),
        in_specs=[vmem],
        out_specs=vmem,
        scratch_shapes=[
            pltpu.SemaphoreType.DMA((columns // piece * share,)),
            pltpu.SemaphoreType.DMA((slots,)),
            pltpu.SemaphoreType.DMA,
        ],
        compiler_params=pltpu.CompilerParams(
            collective_id=collective_id, has_side_effects=True, vmem_limit_bytes=VMEM_LIMIT
        ),
    )(act)


def shifted(shard, axis, by):
    peers = lax.axis_size(axis)
    pairs = [(i, i + by) for i in range(peers) if 0 <= i + by < peers]
    return lax.ppermute(shard, axis, pairs)


def states_kernel(n, own_ref, total_ref, states_ref, totals_ref, sends, recvs, tot_sends, tot_recvs):
    place = lax.axis_index("seq")
    greet("seq", range(1, n))

    def state_copy(offset):
        return pltpu.make_async_remote_copy(
            src_ref=own_ref,
            dst_ref=states_ref.at[offset - 1],
            send_sem=sends.at[offset - 1],
            recv_sem=recvs.at[offset - 1],
            device_id={"seq": lax.rem(place + offset, n)},
            device_id_type=MESH,
        )

    def total_copy(offset):
        return pltpu.make_async_remote_copy(
            src_ref=total_ref,
            dst_ref=totals_ref.at[offset - 1],
            send_sem=tot_sends.at[offset - 1],
            recv_sem=tot_recvs.at[offset - 1],
            device_id={"seq": lax.rem(place + offset, n)},
            device_id_type=MESH,
        )

    for offset in range(1, n):

        @pl.when(place + offset < n)
        def _():
            total_copy(offset).start()
            state_copy(offset).start()

    for offset in range(1, n):

        @pl.when(place < offset)
        def _():
            states_ref[offset - 1] = jnp.zeros(own_ref.shape, own_ref.dtype)
            totals_ref[offset - 1] = jnp.zeros(total_ref.shape, total_ref.dtype)

        @pl.when(place >= offset)
        def _():
            total_copy(offset).wait_recv()
            state_copy(offset).wait_recv()

        @pl.when(place + offset < n)
        def _():
            total_copy(offset).wait_send()
            state_copy(offset).wait_send()


def entering(log_total, state, collective_id):
    n = lax.axis_size("seq")
    heads = log_total.shape[0]
    lanes = -(-heads // 128) * 128
    total = jnp.broadcast_to(jnp.pad(log_total, (0, lanes - heads))[None], (8, lanes))
    own = state.reshape(-1, state.shape[-1]).astype(jnp.bfloat16)
    vmem = pl.BlockSpec(memory_space=pltpu.VMEM)
    sems = pltpu.SemaphoreType.DMA((n - 1,))
    states, totals = pl.pallas_call(
        functools.partial(states_kernel, n),
        out_shape=(
            jax.ShapeDtypeStruct((n - 1, *own.shape), own.dtype),
            jax.ShapeDtypeStruct((n - 1, 8, lanes), jnp.float32),
        ),
        in_specs=[vmem] * 2,
        out_specs=(vmem, vmem),
        scratch_shapes=[sems] * 4,
        compiler_params=pltpu.CompilerParams(
            collective_id=collective_id, has_side_effects=True, vmem_limit_bytes=VMEM_LIMIT
        ),
    )(own, total)
    logs = totals[:, 0, :heads]
    between = jnp.exp(jnp.cumsum(jnp.pad(logs, ((1, 0), (0, 0))), axis=0)[:-1])
    result = jnp.zeros(state.shape, jnp.float32)
    for slot in range(n - 1):
        result = result + between[slot][:, None, None] * states[slot].reshape(state.shape).astype(
            jnp.float32
        )
    return result


def depthwise(rim_rows, current, weights):
    joined = jnp.concatenate([rim_rows, current], axis=0).astype(jnp.float32)
    length = current.shape[0]
    result = jnp.zeros(current.shape, jnp.float32)
    for offset in range(weights.shape[0]):
        result = result + weights[offset] * joined[offset : offset + length]
    return jax.nn.silu(result).astype(jnp.bfloat16)


def on_device(
    hidden,
    norm_gain,
    rank_down,
    gate_up,
    value_up,
    state_up,
    step_up,
    conv_value,
    conv_state,
    step_bias,
    decay_log,
    skip_gain,
    gate_gain,
    out_down,
    out_up,
):
    tokens = hidden.shape[0]
    tp_count = lax.axis_size("tp")
    tp_index = lax.axis_index("tp")
    model_width = hidden.shape[1] * tp_count
    up_weights = (gate_up, value_up, state_up, step_up)
    reduced = project(hidden, rank_down, norm_gain, model_width, 0)
    projected = tuple(
        (jnp.dot(reduced, weight, preferred_element_type=jnp.float32) for weight in up_weights)
    )
    gate_pre = projected[0].astype(jnp.bfloat16)
    value_pre = projected[1].astype(jnp.bfloat16)
    state_pre = projected[2].astype(jnp.bfloat16)
    step_pre = projected[3].astype(jnp.bfloat16)
    rim_start = tokens - conv_value.shape[0] + 1
    rim_value, rim_state = shifted((value_pre[rim_start:], state_pre[rim_start:]), "seq", 1)
    value_act = depthwise(rim_value, value_pre, conv_value)
    state_act = depthwise(rim_state, state_pre, conv_state)
    heads_local = decay_log.shape[0]
    heads_total = heads_local * tp_count
    group_index = tp_index * heads_local // (heads_total // GROUPS)
    sides = exchange(state_act, 1)
    half = sides.shape[0] // 2
    inward = jnp.concatenate([sides[i] for i in range(half)], axis=1)
    outward = jnp.concatenate([sides[half + i] for i in range(half)], axis=1)
    step_size = jax.nn.softplus(step_pre.astype(jnp.float32) + step_bias)
    log_decay = jnp.cumsum(-jnp.exp(decay_log) * step_size, axis=0)
    values = value_act.astype(jnp.float32).reshape(tokens, heads_local, HEAD_DIM)
    coupling = lax.dot_general(
        outward, inward, (((1,), (1,)), ((), ())), preferred_element_type=jnp.float32
    )
    positions = jnp.arange(tokens)
    causal = positions[:, None] >= positions[None, :]
    spread = log_decay.T[:, :, None] - log_decay.T[:, None, :]
    attenuation = jnp.where(causal[None], jnp.exp(jnp.where(causal[None], spread, 0.0)), 0.0)
    mixing = coupling[None] * attenuation * step_size.T[:, None, :]
    narrow_values = value_act.reshape(tokens, heads_local, HEAD_DIM)
    within = jnp.einsum(
        "hts,shp->thp",
        mixing.astype(jnp.bfloat16),
        narrow_values,
        preferred_element_type=jnp.float32,
    )
    ending = jnp.exp(log_decay[-1][None, :] - log_decay) * step_size
    weighted = (ending[:, :, None] * values).astype(jnp.bfloat16)
    local_state = jnp.einsum("shp,sn->hpn", weighted, inward, preferred_element_type=jnp.float32)
    incoming = entering(log_decay[-1], local_state, 3)
    carried_in = jnp.exp(log_decay)[:, :, None] * jnp.einsum(
        "tn,hpn->thp",
        outward,
        incoming.astype(jnp.bfloat16),
        preferred_element_type=jnp.float32,
    )
    mixed = (within + carried_in + skip_gain[None, :, None] * values).reshape(
        tokens, heads_local * HEAD_DIM
    )
    gated = mixed * jax.nn.silu(gate_pre.astype(jnp.float32))
    group_width = heads_total * HEAD_DIM // GROUPS
    own_sum = jnp.sum(gated * gated, axis=1)
    if heads_local * HEAD_DIM < group_width:
        selector = (jnp.arange(GROUPS) == group_index).astype(jnp.float32)
        group_sums = lax.psum(own_sum[:, None] * selector[None, :], "tp")
        own_sum = jnp.sum(group_sums * selector[None, :], axis=1)
    normed = (gated * lax.rsqrt(own_sum / group_width + epsilon)[:, None] * gate_gain).astype(
        jnp.bfloat16
    )
    shared = project(normed, out_down, None, None, 2)
    update = jnp.dot(shared, out_up, preferred_element_type=jnp.float32)
    return (hidden.astype(jnp.float32) + update).astype(jnp.bfloat16)


def solution(mesh):
    return jax.shard_map(
        on_device,
        mesh=mesh,
        in_specs=(
            P("seq", "tp"),
            P("tp"),
            P("tp", None),
            P(None, "tp"),
            P(None, "tp"),
            P(None, "tp"),
            P(None, "tp"),
            P(None, "tp"),
            P(None, "tp"),
            P("tp"),
            P("tp"),
            P("tp"),
            P("tp"),
            P("tp", None),
            P(None, "tp"),
        ),
        out_specs=P("seq", "tp"),
        check_vma=False,
    )
```
